32 devices in a mesh: cfg: 2 (over y), ta: 4 (over z), sa: 2 (over x), src: 2 (over core).
Axes of the slice: x: 2, y: 2, z: 4, core: 2. Of those that a mesh axis runs over, the one named last changes fastest.
Arguments:
- prop: bfloat16 [4, 8, 2, 12, 12, 512], P(('cfg', 'src'), 'ta', None, None, None, 'sa'), parts along dimension 0, may hold values from -6 to 6
- eps_rows: int32 [24, 3], replicated, may hold values from 0 to 11
- eps_sign: int32 [24], replicated, may hold values from 0 to 1
- source_sites: int32 [4, 3], P('cfg'), parts along dimension 0, may hold values from 0 to 15, as said below
- momenta: int32 [8, 3], replicated, may hold values from -2 to 2
Outputs:
- blocks: float32 [4, 8, 2, 8, 1728], P('cfg', None, None, 'ta', 'sa'), parts along dimension 0
The draws below stay inside these ranges and needn't reach their ends.
There are 2 independent parts, one for each index of `cfg`. The reference program is written for one: setup_inputs(seed, part) draws one part's arguments, and reference() takes and returns one part's arrays. A program takes and returns all parts, laid end to end along the dimension named above; an argument that names none is the same for every part. Nothing has to cross between parts.
Inputs may be any that keep to these rules, and one draw needn't show every extreme that they name: `source_sites`: each row is a lattice site: first coordinate below 2, second below 16, third below 16.
All inputs are finite; a program needn't handle non-finite values.
Results may differ from the reference program's by a relative error of at most 0.0045.
Values sent between devices are 32-bit elements; how exact they have to be, the bound alone decides.
No kernel may reach another device: no remote copies, remote signals or barrier semaphores. Data moves between devices by JAX's collectives and lax.ppermute only.
A program may use at most 128 MiB of HBM per device.

```python
import math
import jax
import jax.numpy as jnp
from jax import lax

SC = 12
TERMS = 24
LY = 16
LZ = 16
BLOCK = 1728
LX = 2
SITES = 512
TIMES = 8
NSRC = 2
MOM = 8


def draw_source_sites(key, part):
    key_x = jax.random.fold_in(key, 11)
    key_y = jax.random.fold_in(key, 12)
    key_z = jax.random.fold_in(key, 13)
    key_pick = jax.random.fold_in(key, 14)
    first = jax.random.randint(key_x, (NSRC,), 0, LX)
    second = jax.random.randint(key_y, (NSRC,), 0, LY)
    third = jax.random.randint(key_z, (NSRC,), 0, LZ)
    chosen = jax.random.randint(key_pick, (), 0, NSRC)
    follower = (chosen + 1) % NSRC
    rows = jnp.arange(NSRC, dtype=jnp.int32)
    corner = rows == chosen
    first = jnp.where(corner, LX - 1, first)
    second = jnp.where(corner, LY - 1, second)
    third = jnp.where(corner, LZ - 1, third)
    third = jnp.where(rows == follower, 0, third)
    return jnp.stack([first, second, third], axis=1).astype(jnp.int32)


def set_ends(entries, stream_key, least, top_value):
    longest = entries.shape.index(max(entries.shape))
    spots = []
    for shift in (0, 1):
        where = [jax.random.randint(jax.random.fold_in(stream_key, axis), (), 0, length) for axis, length in enumerate(entries.shape)]
        where[longest] = (where[longest] + shift) % entries.shape[longest]
        spots.append(tuple(where))
    return entries.at[spots[0]].set(least).at[spots[1]].set(top_value)


def shard_levels(stream_key, dims, shards, least, top_value):
    def one(axis_at, shards_of):
        steps = jax.random.uniform(jax.random.fold_in(jax.random.fold_in(stream_key, 6), axis_at), (shards_of,), jnp.float32, least / len(shards), top_value / len(shards))
        return jnp.repeat(jnp.exp(steps), dims[axis_at] // shards_of).reshape((-1,) + (1,) * (len(dims) - axis_at - 1))

    loudness = one(*shards[0])
    for cut in shards[1:]:
        loudness = loudness * one(*cut)
    return loudness


def normal_values(stream_key, dims, deviation, limit, pieces=(), kind=jnp.bfloat16):
    array = jax.random.normal(stream_key, dims, jnp.float32) * deviation
    if len(pieces) > 0:
        array = shard_levels(stream_key, dims, pieces, -0.22, 0.18) * array
    return jnp.clip(array, min=-limit, max=limit).astype(kind)


def setup_inputs(seed: int = 0, part: int = 0) -> dict:
    keys = jax.random.split(jax.random.key(seed), 6)
    part_splits = jax.random.split(jax.random.fold_in(keys[5], part), 6)
    return {
        "prop": normal_values(part_splits[0], (NSRC, TIMES, 2, SC, SC, SITES), 1.0, 6.0, ((0, 2), (1, 4), (5, 2))),
        "eps_rows": set_ends(jax.random.randint(keys[1], (TERMS, 3), 0, SC), jax.random.fold_in(keys[1], 1), 0, SC - 1).astype(jnp.int32),
        "eps_sign": set_ends(jax.random.randint(keys[2], (TERMS,), 0, 2), jax.random.fold_in(keys[2], 1), 0, 1).astype(jnp.int32),
        "source_sites": draw_source_sites(jax.random.fold_in(jax.random.fold_in(keys[5], part), 71), part),
        "momenta": set_ends(jax.random.randint(keys[4], (MOM, 3), -2, 3), jax.random.fold_in(keys[4], 1), -2, 2).astype(jnp.int32),
    }


def phase_table(position, momenta, site_index, extent_x):
    coord_x = site_index // (LY * LZ)
    coord_y = site_index // LZ % LY
    coord_z = site_index % LZ
    part_x = momenta[:, 0:1] * (coord_x[None, :] - position[0]) % extent_x
    part_y = momenta[:, 1:2] * (coord_y[None, :] - position[1]) % LY
    part_z = momenta[:, 2:3] * (coord_z[None, :] - position[2]) % LZ
    angle = 2.0 * math.pi * (part_x.astype(jnp.float32) / extent_x + part_y.astype(jnp.float32) / LY + part_z.astype(jnp.float32) / LZ)
    return jnp.concatenate([jnp.cos(angle), jnp.sin(angle)], axis=0).astype(jnp.bfloat16)

def contract(slab, rows, weights):
    first = jnp.take(slab, rows[:, 0], axis=1).astype(jnp.float32)
    second = jnp.take(slab, rows[:, 1], axis=1).astype(jnp.float32)
    third = jnp.take(slab, rows[:, 2], axis=1)
    scaled = weights[:, None, None, None]
    real = scaled * (first[0][:, :, None] * second[0][:, None] - first[1][:, :, None] * second[1][:, None])
    imag = scaled * (first[0][:, :, None] * second[1][:, None] + first[1][:, :, None] * second[0][:, None])
    pair = jnp.stack([real, imag]).astype(jnp.bfloat16)
    mixer = jnp.stack([jnp.stack([third[0], -third[1]]), jnp.stack([third[1], third[0]])])
    block = jnp.einsum('ceijx,oceLx->oijLx', pair.astype(jnp.float32), mixer.astype(jnp.float32))
    width = slab.shape[1]
    return block.astype(jnp.bfloat16).reshape(2 * width * width * width, slab.shape[-1])

def mix_phase(table, quark):
    product = jnp.dot(table, quark.T, preferred_element_type=jnp.float32)
    half_m = table.shape[0] // 2
    half_k = quark.shape[0] // 2
    cos_re = product[:half_m, :half_k]
    cos_im = product[:half_m, half_k:]
    sin_re = product[half_m:, :half_k]
    sin_im = product[half_m:, half_k:]
    return jnp.stack([cos_re + sin_im, cos_im - sin_re])

def reference(prop, eps_rows, eps_sign, source_sites, momenta):
    weights = (2 * eps_sign - 1).astype(jnp.float32)
    scale = 1.0 / math.sqrt(4.0 * TERMS * SITES)
    site_index = jnp.arange(SITES, dtype=jnp.int32)
    tables = jnp.stack([phase_table(source_sites[s], momenta, site_index, LX) for s in range(NSRC)])
    slabs = prop.reshape((NSRC * TIMES,) + prop.shape[2:])
    owners = jnp.repeat(jnp.arange(NSRC, dtype=jnp.int32), TIMES)

    def project(items):
        slab, owner = items
        quark = contract(slab, eps_rows, weights)
        return scale * mix_phase(tables[owner], quark)
    result = lax.map(project, (slabs, owners))
    return result.reshape(NSRC, TIMES, 2, MOM, BLOCK)
```

```python
import math

import jax
import jax.numpy as jnp
from jax import lax
from jax.experimental import pallas as pl
from jax.experimental.pallas import tpu as pltpu
from jax.sharding import PartitionSpec as P

LY = 16
LZ = 16
GROUP = 4


def wrap(value, length):
    if length & (length - 1) == 0:
        return value & (length - 1)
    return jnp.mod(value, length)


def project_kernel(rows, signs, sites, momenta, prop, out, spread, tiled, phased, pairs, total, *,
                   times, site_count, sites_total, scale):
    step = pl.program_id(0)
    width = prop.shape[2]
    mom = momenta.shape[0]
    terms = rows.shape[0]
    extent_x = sites_total // (LY * LZ)
    per = mom * width
    square = width * width

    owner = lax.axis_index("src") * (pl.num_programs(0) // times) + step // times
    site = lax.axis_index("sa") * site_count + lax.broadcasted_iota(jnp.int32, (mom, site_count), 1)
    coord_x = site // (LY * LZ)
    coord_y = wrap(site // LZ, LY)
    coord_z = wrap(site, LZ)
    part_x = wrap(momenta[:, 0:1] * (coord_x - sites[owner, 0]), extent_x)
    part_y = wrap(momenta[:, 1:2] * (coord_y - sites[owner, 1]), LY)
    part_z = wrap(momenta[:, 2:3] * (coord_z - sites[owner, 2]), LZ)
    angle = (2.0 * math.pi) * (
        part_x.astype(jnp.float32) / extent_x
        + part_y.astype(jnp.float32) / LY
        + part_z.astype(jnp.float32) / LZ
    )
    cosine = jnp.cos(angle).astype(jnp.bfloat16).astype(jnp.float32)
    sine = jnp.sin(angle).astype(jnp.bfloat16).astype(jnp.float32)
    low = lax.broadcasted_iota(jnp.int32, (8, site_count), 0) < 4

    def prepare(r, carry):
        parts = [prop[0, c, r].astype(jnp.float32) for c in range(2)]
        for c in range(2):
            tiled[r, c] = jnp.concatenate([parts[c], parts[c]], axis=0)
            for j in range(0, width, 2):
                first = jnp.broadcast_to(parts[c][j:j + 1], (8, site_count))
                second = jnp.broadcast_to(parts[c][j + 1:j + 2], (8, site_count))
                at = j * width
                spread[r, c, at:at + 8] = first
                spread[r, c, at + 8:at + 16] = jnp.where(low, first, second)
                spread[r, c, at + 16:at + 24] = second
        for i in range(0, width, 2):
            reals = []
            imags = []
            for q in (i, i + 1):
                re = jnp.broadcast_to(parts[0][q:q + 1], (mom, site_count))
                im = jnp.broadcast_to(parts[1][q:q + 1], (mom, site_count))
                reals.append(re * cosine + im * sine)
                imags.append(im * cosine - re * sine)
            real = jnp.concatenate(reals, axis=0).astype(jnp.bfloat16)
            imag = jnp.concatenate(imags, axis=0)
            minus = (-imag).astype(jnp.bfloat16)
            imag = imag.astype(jnp.bfloat16)
            at = i * mom
            phased[r, at:at + 2 * mom, :site_count] = real
            phased[r, at:at + 2 * mom, site_count:] = minus
            phased[r, per + at:per + at + 2 * mom, :site_count] = imag
            phased[r, per + at:per + at + 2 * mom, site_count:] = real
        return carry

    lax.fori_loop(0, width, prepare, 0)
    total[...] = jnp.zeros_like(total)

    def accumulate(block, carry):
        left = []
        for u in range(GROUP):
            e = block * GROUP + u
            r1 = rows[e, 1]
            r2 = rows[e, 2]
            weight = (2 * signs[e] - 1).astype(jnp.float32)
            re2 = tiled[r2, 0] * weight
            im2 = tiled[r2, 1] * weight
            re2 = jnp.concatenate([re2, re2], axis=0)
            im2 = jnp.concatenate([im2, im2], axis=0)
            at = u * 2 * site_count
            for j in range(0, square, 4 * width):
                re1 = spread[r1, 0, j:j + 4 * width]
                im1 = spread[r1, 1, j:j + 4 * width]
                pairs[j:j + 4 * width, at:at + site_count] = (re1 * re2 - im1 * im2).astype(jnp.bfloat16)
                pairs[j:j + 4 * width, at + site_count:at + 2 * site_count] = (
                    re1 * im2 + im1 * re2
                ).astype(jnp.bfloat16)
            left.append(phased[rows[e, 0]])
        total[...] += lax.dot_general(
            jnp.concatenate(left, axis=1), pairs[...], (((1,), (1,)), ((), ())),
            preferred_element_type=jnp.float32,
        )
        return carry

    lax.fori_loop(0, terms // GROUP, accumulate, 0)

    owners = out.shape[0]
    mine = out.shape[3]
    span = out.shape[4] // square
    halves = width // span
    for c in range(2):
        for i in range(width):
            value = total[c * per + i * mom:c * per + (i + 1) * mom] * scale
            half = i // span
            at = (i % span) * square
            for a in range(owners // halves):
                out[a * halves + half, 0, c, :, at:at + square] = value[a * mine:(a + 1) * mine]


def per_device(prop, eps_rows, eps_sign, source_sites, momenta):
    src_count, time_count = prop.shape[:2]
    width = prop.shape[3]
    site_count = prop.shape[5]
    sites_total = site_count * lax.axis_size("sa")
    mom = momenta.shape[0]
    terms = eps_rows.shape[0]
    scale = 1.0 / math.sqrt(4.0 * terms * sites_total)
    slabs = prop.reshape((src_count * time_count,) + prop.shape[2:])
    owners = lax.axis_size("ta") * lax.axis_size("sa")
    mine = mom // lax.axis_size("ta")
    span = width ** 3 // lax.axis_size("sa")

    def body(*refs):
        project_kernel(*refs, times=time_count, site_count=site_count, sites_total=sites_total, scale=scale)

    smem = pl.BlockSpec(memory_space=pltpu.SMEM)
    partial_value = pl.pallas_call(
        body,
        grid=(slabs.shape[0],),
        in_specs=[
            smem, smem, smem,
            pl.BlockSpec(momenta.shape, lambda s: (0, 0)),
            pl.BlockSpec((1,) + slabs.shape[1:], lambda s: (s, 0, 0, 0, 0)),
        ],
        out_specs=pl.BlockSpec((owners, 1, 2, mine, span), lambda s: (0, s, 0, 0, 0)),
        out_shape=jax.ShapeDtypeStruct((owners, slabs.shape[0], 2, mine, span), jnp.float32),
        scratch_shapes=[
            pltpu.VMEM((width, 2, width * width, site_count), jnp.float32),
            pltpu.VMEM((width, 2, 2 * width, site_count), jnp.float32),
            pltpu.VMEM((width, 2 * width * mom, 2 * site_count), jnp.bfloat16),
            pltpu.VMEM((width * width, GROUP * 2 * site_count), jnp.bfloat16),
            pltpu.VMEM((2 * width * mom, width * width), jnp.float32),
        ],
        name="project",
    )(eps_rows, eps_sign, source_sites, momenta, slabs)

    moved = lax.all_to_all(partial_value, ("ta", "sa"), split_axis=0, concat_axis=0, tiled=True)
    moved = moved.reshape((lax.axis_size("ta"), lax.axis_size("sa")) + moved.shape[1:])
    summed = jnp.sum(moved, axis=1)
    summed = summed.reshape((lax.axis_size("ta"), src_count, time_count) + summed.shape[2:])
    summed = jnp.moveaxis(summed, 1, 0).reshape((src_count, -1) + summed.shape[3:])
    return lax.all_gather(summed, "src", axis=0, tiled=True)


def solution(mesh):
    return jax.shard_map(
        per_device,
        mesh=mesh,
        in_specs=(P(("cfg", "src"), "ta", None, None, None, "sa"), P(), P(), P("cfg", None), P()),
        out_specs=P("cfg", None, None, "ta", "sa"),
        check_vma=False,
    )
```

```python
import math

import jax
import jax.numpy as jnp
from jax import lax
from jax.experimental import pallas as pl
from jax.experimental.pallas import tpu as pltpu
from jax.sharding import PartitionSpec as P

LY = 16
LZ = 16
GROUP = 4


def wrap(value, length):
    if length & (length - 1) == 0:
        return value & (length - 1)
    return jnp.mod(value, length)


def project_kernel(rows, signs, sites, momenta, prop, out, spread, tiled, phased, pairs, total, table, *,
                   times, site_count, sites_total, scale):
    step = pl.program_id(0)
    width = prop.shape[1]
    mom = momenta.shape[1]
    terms = rows.shape[1]
    extent_x = sites_total // (LY * LZ)
    per = mom * width
    square = width * width

    @pl.when(step % times == 0)
    def _():
        owner = lax.axis_index("src") * (pl.num_programs(0) // times) + step // times
        site = lax.axis_index("sa") * site_count + lax.broadcasted_iota(jnp.int32, (mom, site_count), 1)
        row = lax.broadcasted_iota(jnp.int32, (mom, site_count), 0)
        coords = (site // (LY * LZ), wrap(site // LZ, LY), wrap(site, LZ))
        lengths = (extent_x, LY, LZ)
        turns = []
        for d in range(3):
            factor = jnp.zeros((mom, site_count), jnp.int32)
            for p in range(mom):
                factor = jnp.where(row == p, momenta[d, p], factor)
            part = wrap(factor * (coords[d] - sites[owner, d]), lengths[d])
            turns.append(part.astype(jnp.float32) / lengths[d])
        angle = (2.0 * math.pi) * (turns[0] + turns[1] + turns[2])
        table[0] = jnp.cos(angle).astype(jnp.bfloat16).astype(jnp.float32)
        table[1] = jnp.sin(angle).astype(jnp.bfloat16).astype(jnp.float32)

    cosine = table[0]
    sine = table[1]
    low = lax.broadcasted_iota(jnp.int32, (8, site_count), 0) < 4

    def prepare(r, carry):
        both = prop[0, r].astype(jnp.float32)
        parts = [both[:, c] for c in range(2)]
        for c in range(2):
            tiled[r, c] = jnp.concatenate([parts[c], parts[c]], axis=0)
            for j in range(0, width, 2):
                first = jnp.broadcast_to(parts[c][j:j + 1], (8, site_count))
                second = jnp.broadcast_to(parts[c][j + 1:j + 2], (8, site_count))
                at = j * width
                spread[r, c, at:at + 8] = first
                spread[r, c, at + 8:at + 16] = jnp.where(low, first, second)
                spread[r, c, at + 16:at + 24] = second
        for i in range(0, width, 2):
            reals = []
            imags = []
            for q in (i, i + 1):
                re = jnp.broadcast_to(parts[0][q:q + 1], (mom, site_count))
                im = jnp.broadcast_to(parts[1][q:q + 1], (mom, site_count))
                reals.append(re * cosine + im * sine)
                imags.append(im * cosine - re * sine)
            real = jnp.concatenate(reals, axis=0).astype(jnp.bfloat16)
            imag = jnp.concatenate(imags, axis=0)
            minus = (-imag).astype(jnp.bfloat16)
            imag = imag.astype(jnp.bfloat16)
            at = i * mom
            phased[r, at:at + 2 * mom, :site_count] = real
            phased[r, at:at + 2 * mom, site_count:] = minus
            phased[r, per + at:per + at + 2 * mom, :site_count] = imag
            phased[r, per + at:per + at + 2 * mom, site_count:] = real
        return carry

    lax.fori_loop(0, width, prepare, 0)
    total[...] = jnp.zeros_like(total)

    def accumulate(block, carry):
        left = []
        for u in range(GROUP):
            e = block * GROUP + u
            r1 = rows[1, e]
            r2 = rows[2, e]
            weight = (2 * signs[e] - 1).astype(jnp.float32)
            re2 = tiled[r2, 0] * weight
            im2 = tiled[r2, 1] * weight
            re2 = jnp.concatenate([re2, re2], axis=0)
            im2 = jnp.concatenate([im2, im2], axis=0)
            at = u * 2 * site_count
            for j in range(0, square, 4 * width):
                re1 = spread[r1, 0, j:j + 4 * width]
                im1 = spread[r1, 1, j:j + 4 * width]
                pairs[j:j + 4 * width, at:at + site_count] = (re1 * re2 - im1 * im2).astype(jnp.bfloat16)
                pairs[j:j + 4 * width, at + site_count:at + 2 * site_count] = (
                    re1 * im2 + im1 * re2
                ).astype(jnp.bfloat16)
            left.append(phased[rows[0, e]])
        total[...] += lax.dot_general(
            jnp.concatenate(left, axis=1), pairs[...], (((1,), (1,)), ((), ())),
            preferred_element_type=jnp.float32,
        )
        return carry

    lax.fori_loop(0, terms // GROUP, accumulate, 0)

    owners = out.shape[0]
    mine = out.shape[3]
    span = out.shape[4] // square
    halves = width // span
    for c in range(2):
        for i in range(width):
            value = total[c * per + i * mom:c * per + (i + 1) * mom] * scale
            half = i // span
            at = (i % span) * square
            for a in range(owners // halves):
                out[a * halves + half, 0, c, :, at:at + square] = value[a * mine:(a + 1) * mine]


def per_device(prop, eps_rows, eps_sign, source_sites, momenta):
    src_count, time_count = prop.shape[:2]
    width = prop.shape[3]
    site_count = prop.shape[5]
    sites_total = site_count * lax.axis_size("sa")
    mom = momenta.shape[0]
    terms = eps_rows.shape[0]
    scale = 1.0 / math.sqrt(4.0 * terms * sites_total)
    slabs = jnp.transpose(prop, (0, 1, 3, 4, 2, 5))
    slabs = slabs.reshape((src_count * time_count,) + slabs.shape[2:])
    owners = lax.axis_size("ta") * lax.axis_size("sa")
    mine = mom // lax.axis_size("ta")
    span = width ** 3 // lax.axis_size("sa")

    def body(*refs):
        project_kernel(*refs, times=time_count, site_count=site_count, sites_total=sites_total, scale=scale)

    smem = pl.BlockSpec(memory_space=pltpu.SMEM)
    partial_value = pl.pallas_call(
        body,
        grid=(slabs.shape[0],),
        in_specs=[
            smem, smem, smem, smem,
            pl.BlockSpec((1,) + slabs.shape[1:], lambda s: (s, 0, 0, 0, 0)),
        ],
        out_specs=pl.BlockSpec((owners, 1, 2, mine, span), lambda s: (0, s, 0, 0, 0)),
        out_shape=jax.ShapeDtypeStruct((owners, slabs.shape[0], 2, mine, span), jnp.float32),
        scratch_shapes=[
            pltpu.VMEM((width, 2, width * width, site_count), jnp.float32),
            pltpu.VMEM((width, 2, 2 * width, site_count), jnp.float32),
            pltpu.VMEM((width, 2 * width * mom, 2 * site_count), jnp.bfloat16),
            pltpu.VMEM((width * width, GROUP * 2 * site_count), jnp.bfloat16),
            pltpu.VMEM((2 * width * mom, width * width), jnp.float32),
            pltpu.VMEM((2, mom, site_count), jnp.float32),
        ],
        name="project",
    )(eps_rows.T, eps_sign, source_sites, momenta.T, slabs)

    moved = lax.all_to_all(partial_value, ("ta", "sa"), split_axis=0, concat_axis=0, tiled=True)
    moved = moved.reshape((lax.axis_size("ta"), lax.axis_size("sa")) + moved.shape[1:])
    summed = jnp.sum(moved, axis=1)
    summed = summed.reshape((lax.axis_size("ta"), src_count, time_count) + summed.shape[2:])
    summed = jnp.moveaxis(summed, 1, 0).reshape((src_count, -1) + summed.shape[3:])
    return lax.all_gather(summed, "src", axis=0, tiled=True)


def solution(mesh):
    return jax.shard_map(
        per_device,
        mesh=mesh,
        in_specs=(P(("cfg", "src"), "ta", None, None, None, "sa"), P(), P(), P("cfg", None), P()),
        out_specs=P("cfg", None, None, "ta", "sa"),
        check_vma=False,
    )
```

```python
import math

import jax
import jax.numpy as jnp
from jax import lax
from jax.experimental import pallas as pl
from jax.experimental.pallas import tpu as pltpu
from jax.sharding import PartitionSpec as P

LY = 16
LZ = 16
GROUP = 4


def wrap(value, length):
    if length & (length - 1) == 0:
        return value & (length - 1)
    return jnp.mod(value, length)


def project_kernel(rows, signs, sites, momenta, prop, out, tiled, phased, pairs, total, table, *,
                   times, site_count, sites_total, scale):
    step = pl.program_id(0)
    width = prop.shape[1]
    mom = momenta.shape[1]
    terms = rows.shape[1]
    extent_x = sites_total // (LY * LZ)
    per = mom * width
    square = width * width

    @pl.when(step % times == 0)
    def _():
        owner = lax.axis_index("src") * (pl.num_programs(0) // times) + step // times
        site = lax.axis_index("sa") * site_count + lax.broadcasted_iota(jnp.int32, (mom, site_count), 1)
        row = lax.broadcasted_iota(jnp.int32, (mom, site_count), 0)
        coords = (site // (LY * LZ), wrap(site // LZ, LY), wrap(site, LZ))
        lengths = (extent_x, LY, LZ)
        turns = []
        for d in range(3):
            factor = jnp.zeros((mom, site_count), jnp.int32)
            for p in range(mom):
                factor = jnp.where(row == p, momenta[d, p], factor)
            part = wrap(factor * (coords[d] - sites[owner, d]), lengths[d])
            turns.append(part.astype(jnp.float32) / lengths[d])
        angle = (2.0 * math.pi) * (turns[0] + turns[1] + turns[2])
        table[0] = jnp.cos(angle).astype(jnp.bfloat16).astype(jnp.float32)
        table[1] = jnp.sin(angle).astype(jnp.bfloat16).astype(jnp.float32)

    cosine = table[0]
    sine = table[1]
    low = lax.broadcasted_iota(jnp.int32, (8, site_count), 0) < 4

    def prepare(r, carry):
        both = prop[0, r].astype(jnp.float32)
        parts = [both[:, c] for c in range(2)]
        for c in range(2):
            tiled[r, c] = jnp.concatenate([parts[c], parts[c]], axis=0)
        for i in range(0, width, 2):
            reals = []
            imags = []
            for q in (i, i + 1):
                re = jnp.broadcast_to(parts[0][q:q + 1], (mom, site_count))
                im = jnp.broadcast_to(parts[1][q:q + 1], (mom, site_count))
                reals.append(re * cosine + im * sine)
                imags.append(im * cosine - re * sine)
            real = jnp.concatenate(reals, axis=0).astype(jnp.bfloat16)
            imag = jnp.concatenate(imags, axis=0)
            minus = (-imag).astype(jnp.bfloat16)
            imag = imag.astype(jnp.bfloat16)
            at = i * mom
            phased[r, at:at + 2 * mom, :site_count] = real
            phased[r, at:at + 2 * mom, site_count:] = minus
            phased[r, per + at:per + at + 2 * mom, :site_count] = imag
            phased[r, per + at:per + at + 2 * mom, site_count:] = real
        return carry

    lax.fori_loop(0, width, prepare, 0)
    total[...] = jnp.zeros_like(total)

    def accumulate(block, carry):
        left = []
        for u in range(GROUP):
            e = block * GROUP + u
            r1 = rows[1, e]
            r2 = rows[2, e]
            weight = (2 * signs[e] - 1).astype(jnp.float32)
            re2 = tiled[r2, 0] * weight
            im2 = tiled[r2, 1] * weight
            at = u * 2 * site_count
            for j in range(0, width, 4):
                reals = []
                imags = []
                for q in (j, j + 2):
                    ends = [
                        [tiled[r1, c, pl.ds(k, 8, stride=0)] for k in (q, q + 1)] for c in range(2)
                    ]
                    mixed = [jnp.where(low, ends[c][0], ends[c][1]) for c in range(2)]
                    for v, (re1, im1) in enumerate(
                        ((ends[0][0], ends[1][0]), (mixed[0], mixed[1]), (ends[0][1], ends[1][1]))
                    ):
                        re = re2[8 * v:8 * v + 8]
                        im = im2[8 * v:8 * v + 8]
                        reals.append(re1 * re - im1 * im)
                        imags.append(re1 * im + im1 * re)
                span = slice(j * width, (j + 4) * width)
                pairs[span, at:at + site_count] = jnp.concatenate(reals, axis=0).astype(jnp.bfloat16)
                pairs[span, at + site_count:at + 2 * site_count] = (
                    jnp.concatenate(imags, axis=0).astype(jnp.bfloat16)
                )
            left.append(phased[rows[0, e]])
        total[...] += lax.dot_general(
            jnp.concatenate(left, axis=1), pairs[...], (((1,), (1,)), ((), ())),
            preferred_element_type=jnp.float32,
        )
        return carry

    lax.fori_loop(0, terms // GROUP, accumulate, 0)

    owners = out.shape[0]
    mine = out.shape[3]
    span = out.shape[4] // square
    halves = width // span
    for c in range(2):
        for i in range(width):
            value = total[c * per + i * mom:c * per + (i + 1) * mom] * scale
            half = i // span
            at = (i % span) * square
            for a in range(owners // halves):
                out[a * halves + half, step, c, :, at:at + square] = value[a * mine:(a + 1) * mine]


def per_device(prop, eps_rows, eps_sign, source_sites, momenta):
    src_count, time_count = prop.shape[:2]
    width = prop.shape[3]
    site_count = prop.shape[5]
    sites_total = site_count * lax.axis_size("sa")
    mom = momenta.shape[0]
    terms = eps_rows.shape[0]
    scale = 1.0 / math.sqrt(4.0 * terms * sites_total)
    slabs = jnp.transpose(prop, (0, 1, 3, 4, 2, 5))
    slabs = slabs.reshape((src_count * time_count,) + slabs.shape[2:])
    owners = lax.axis_size("ta") * lax.axis_size("sa")
    mine = mom // lax.axis_size("ta")
    span = width ** 3 // lax.axis_size("sa")

    def body(*refs):
        project_kernel(*refs, times=time_count, site_count=site_count, sites_total=sites_total, scale=scale)

    smem = pl.BlockSpec(memory_space=pltpu.SMEM)
    partial_value = pl.pallas_call(
        body,
        grid=(slabs.shape[0],),
        in_specs=[
            smem, smem, smem, smem,
            pl.BlockSpec((1,) + slabs.shape[1:], lambda s: (s, 0, 0, 0, 0)),
        ],
        out_specs=pl.BlockSpec(memory_space=pltpu.VMEM),
        out_shape=pltpu.VMEM((owners, slabs.shape[0], 2, mine, span), jnp.float32),
        scratch_shapes=[
            pltpu.VMEM((width, 2, 2 * width, site_count), jnp.float32),
            pltpu.VMEM((width, 2 * width * mom, 2 * site_count), jnp.bfloat16),
            pltpu.VMEM((width * width, GROUP * 2 * site_count), jnp.bfloat16),
            pltpu.VMEM((2 * width * mom, width * width), jnp.float32),
            pltpu.VMEM((2, mom, site_count), jnp.float32),
        ],
        name="project",
    )(eps_rows.T, eps_sign, source_sites, momenta.T, slabs)

    moved = lax.all_to_all(partial_value, ("ta", "sa"), split_axis=0, concat_axis=0, tiled=True)
    moved = moved.reshape((lax.axis_size("ta"), lax.axis_size("sa")) + moved.shape[1:])
    summed = jnp.sum(moved, axis=1)
    summed = summed.reshape((lax.axis_size("ta"), src_count, time_count) + summed.shape[2:])
    summed = jnp.moveaxis(summed, 1, 0).reshape((src_count, -1) + summed.shape[3:])
    return lax.all_gather(summed, "src", axis=0, tiled=True)


def solution(mesh):
    return jax.shard_map(
        per_device,
        mesh=mesh,
        in_specs=(P(("cfg", "src"), "ta", None, None, None, "sa"), P(), P(), P("cfg", None), P()),
        out_specs=P("cfg", None, None, "ta", "sa"),
        check_vma=False,
    )
```

```python
import math

import jax
import jax.numpy as jnp
from jax import lax
from jax.experimental import pallas as pl
from jax.experimental.pallas import tpu as pltpu
from jax.sharding import PartitionSpec as P

LY = 16
LZ = 16
GROUP = 24


def wrap(value, length):
    if length & (length - 1) == 0:
        return value & (length - 1)
    return jnp.mod(value, length)


def project_kernel(rows, signs, sites, momenta, prop, out, tiled, phased, pairs, total, table, *,
                   times, site_count, sites_total, scale):
    step = pl.program_id(0)
    width = prop.shape[1]
    mom = momenta.shape[1]
    terms = rows.shape[1]
    extent_x = sites_total // (LY * LZ)
    per = mom * width
    square = width * width

    @pl.when(step % times == 0)
    def _():
        owner = lax.axis_index("src") * (pl.num_programs(0) // times) + step // times
        site = lax.axis_index("sa") * site_count + lax.broadcasted_iota(jnp.int32, (mom, site_count), 1)
        row = lax.broadcasted_iota(jnp.int32, (mom, site_count), 0)
        coords = (site // (LY * LZ), wrap(site // LZ, LY), wrap(site, LZ))
        lengths = (extent_x, LY, LZ)
        turns = []
        for d in range(3):
            factor = jnp.zeros((mom, site_count), jnp.int32)
            for p in range(mom):
                factor = jnp.where(row == p, momenta[d, p], factor)
            part = wrap(factor * (coords[d] - sites[owner, d]), lengths[d])
            turns.append(part.astype(jnp.float32) / lengths[d])
        angle = (2.0 * math.pi) * (turns[0] + turns[1] + turns[2])
        table[0] = jnp.cos(angle).astype(jnp.bfloat16).astype(jnp.float32)
        table[1] = jnp.sin(angle).astype(jnp.bfloat16).astype(jnp.float32)

    cosine = table[0]
    sine = table[1]
    low = lax.broadcasted_iota(jnp.int32, (8, site_count), 0) < 4

    def prepare(r, carry):
        both = prop[0, r].astype(jnp.float32)
        parts = [both[:, c] for c in range(2)]
        for c in range(2):
            tiled[r, c] = jnp.concatenate([parts[c], parts[c]], axis=0)
        for i in range(0, width, 2):
            reals = []
            imags = []
            for q in (i, i + 1):
                re = jnp.broadcast_to(parts[0][q:q + 1], (mom, site_count))
                im = jnp.broadcast_to(parts[1][q:q + 1], (mom, site_count))
                reals.append(re * cosine + im * sine)
                imags.append(im * cosine - re * sine)
            real = jnp.concatenate(reals, axis=0).astype(jnp.bfloat16)
            imag = jnp.concatenate(imags, axis=0)
            minus = (-imag).astype(jnp.bfloat16)
            imag = imag.astype(jnp.bfloat16)
            at = i * mom
            phased[r, at:at + 2 * mom, :site_count] = real
            phased[r, at:at + 2 * mom, site_count:] = minus
            phased[r, per + at:per + at + 2 * mom, :site_count] = imag
            phased[r, per + at:per + at + 2 * mom, site_count:] = real
        return carry

    lax.fori_loop(0, width, prepare, 0)
    group = max(g for g in range(1, GROUP + 1) if terms % g == 0)

    def accumulate(block, carry):
        left = []
        for u in range(group):
            e = block * group + u
            r1 = rows[1, e]
            r2 = rows[2, e]
            weight = (2 * signs[e] - 1).astype(jnp.float32)
            re2 = tiled[r2, 0] * weight
            im2 = tiled[r2, 1] * weight
            at = u * 2 * site_count
            for j in range(0, width, 4):
                reals = []
                imags = []
                for q in (j, j + 2):
                    ends = [
                        [tiled[r1, c, pl.ds(k, 8, stride=0)] for k in (q, q + 1)] for c in range(2)
                    ]
                    mixed = [jnp.where(low, ends[c][0], ends[c][1]) for c in range(2)]
                    for v, (re1, im1) in enumerate(
                        ((ends[0][0], ends[1][0]), (mixed[0], mixed[1]), (ends[0][1], ends[1][1]))
                    ):
                        re = re2[8 * v:8 * v + 8]
                        im = im2[8 * v:8 * v + 8]
                        reals.append(re1 * re - im1 * im)
                        imags.append(re1 * im + im1 * re)
                span = slice(j * width, (j + 4) * width)
                pairs[span, at:at + site_count] = jnp.concatenate(reals, axis=0).astype(jnp.bfloat16)
                pairs[span, at + site_count:at + 2 * site_count] = (
                    jnp.concatenate(imags, axis=0).astype(jnp.bfloat16)
                )
            left.append(phased[rows[0, e]])
        product = lax.dot_general(
            jnp.concatenate(left, axis=1), pairs[:, :group * 2 * site_count], (((1,), (1,)), ((), ())),
            preferred_element_type=jnp.float32,
        )
        if terms == group:
            total[...] = product
        else:
            total[...] += product
        return carry

    if terms == group:
        accumulate(0, 0)
    else:
        total[...] = jnp.zeros_like(total)
        lax.fori_loop(0, terms // group, accumulate, 0)

    owners = out.shape[0]
    mine = out.shape[3]
    span = out.shape[4] // square
    halves = width // span
    for c in range(2):
        for i in range(width):
            value = total[c * per + i * mom:c * per + (i + 1) * mom] * scale
            half = i // span
            at = (i % span) * square
            for a in range(owners // halves):
                out[a * halves + half, step, c, :, at:at + square] = value[a * mine:(a + 1) * mine]


def per_device(prop, eps_rows, eps_sign, source_sites, momenta):
    src_count, time_count = prop.shape[:2]
    width = prop.shape[3]
    site_count = prop.shape[5]
    sites_total = site_count * lax.axis_size("sa")
    mom = momenta.shape[0]
    terms = eps_rows.shape[0]
    scale = 1.0 / math.sqrt(4.0 * terms * sites_total)
    slabs = jnp.transpose(prop, (0, 1, 3, 4, 2, 5))
    slabs = slabs.reshape((src_count * time_count,) + slabs.shape[2:])
    owners = lax.axis_size("ta") * lax.axis_size("sa")
    mine = mom // lax.axis_size("ta")
    span = width ** 3 // lax.axis_size("sa")

    def body(*refs):
        project_kernel(*refs, times=time_count, site_count=site_count, sites_total=sites_total, scale=scale)

    smem = pl.BlockSpec(memory_space=pltpu.SMEM)
    partial_value = pl.pallas_call(
        body,
        grid=(slabs.shape[0],),
        in_specs=[
            smem, smem, smem, smem,
            pl.BlockSpec((1,) + slabs.shape[1:], lambda s: (s, 0, 0, 0, 0)),
        ],
        out_specs=pl.BlockSpec(memory_space=pltpu.VMEM),
        out_shape=pltpu.VMEM((owners, slabs.shape[0], 2, mine, span), jnp.float32),
        scratch_shapes=[
            pltpu.VMEM((width, 2, 2 * width, site_count), jnp.float32),
            pltpu.VMEM((width, 2 * width * mom, 2 * site_count), jnp.bfloat16),
            pltpu.VMEM((width * width, min(GROUP, terms) * 2 * site_count), jnp.bfloat16),
            pltpu.VMEM((2 * width * mom, width * width), jnp.float32),
            pltpu.VMEM((2, mom, site_count), jnp.float32),
        ],
        name="project",
    )(eps_rows.T, eps_sign, source_sites, momenta.T, slabs)

    moved = lax.all_to_all(partial_value, ("ta", "sa"), split_axis=0, concat_axis=0, tiled=True)
    moved = moved.reshape((lax.axis_size("ta"), lax.axis_size("sa")) + moved.shape[1:])
    summed = jnp.sum(moved, axis=1)
    summed = summed.reshape((lax.axis_size("ta"), src_count, time_count) + summed.shape[2:])
    summed = jnp.moveaxis(summed, 1, 0).reshape((src_count, -1) + summed.shape[3:])
    return lax.all_gather(summed, "src", axis=0, tiled=True)


def solution(mesh):
    return jax.shard_map(
        per_device,
        mesh=mesh,
        in_specs=(P(("cfg", "src"), "ta", None, None, None, "sa"), P(), P(), P("cfg", None), P()),
        out_specs=P("cfg", None, None, "ta", "sa"),
        check_vma=False,
    )
```
